256 devices in a mesh: dp: 64 (over z, y, core), vocab: 4 (over x).
Axes of the slice: x: 4, y: 4, z: 8, core: 2. Of those that a mesh axis runs over, the one named last changes fastest.
Arguments:
- hidden_in: bfloat16 [512, 24, 1024], P(('dp', 'vocab')), may hold values from -6 to 6
- tokens: int32 [512, 24], P(('dp', 'vocab')), may hold values from 0 to 131071
- lengths: int32 [512], P(('dp', 'vocab')), may hold values from 2 to 24, as said below
- cutoff: int32 [1], replicated, may hold values from 1 to 512
- norm_gain: float32 [1024], replicated, may hold values from 0.5 to 1.5
- gate_weight: bfloat16 [1024, 4096], P(None, 'vocab'), may hold values from -0.1875 to 0.1875
- up_weight: bfloat16 [1024, 4096], P(None, 'vocab'), may hold values from -0.1875 to 0.1875
- down_weight: bfloat16 [4096, 1024], P('vocab'), may hold values from -0.09375 to 0.09375
- final_gain: float32 [1024], replicated, may hold values from 0.5 to 1.5
- head_table: bfloat16 [131072, 1024], P(('dp', 'vocab')), may hold values from -12 to 12
Outputs:
- log_ppl: float32 [512], P(('dp', 'vocab'))
- margin: float32 [512], P(('dp', 'vocab'))
The draws below stay inside these ranges and needn't reach their ends.
Inputs may be any that keep to these rules, and one draw needn't show every extreme that they name: Every length is 2 or more; the documents of one device have together at most 32 positions below their lengths, and some device has exactly 32.
All inputs are finite; a program needn't handle non-finite values.
Results may differ from the reference program's by a relative error of at most 0.025.
Values may be sent and summed in bfloat16 or wider, within the bound.
No kernel may reach another device: no remote copies, remote signals or barrier semaphores. Data moves between devices by JAX's collectives and lax.ppermute only.
A program may use at most 64 MiB of HBM per device.

```python
import math
import jax
import jax.numpy as jnp
import numpy as np
from jax import lax

D = 1024
FF = 4096
V = 131072
L = 24
CAP = 32
DOCS = 512


def draw_lengths(key, part):
    pairs = DOCS // 2
    keys = jax.random.split(jax.random.fold_in(key, 23), 4)
    former = jax.random.randint(keys[0], (pairs,), 2, L + 1)
    room = jnp.minimum(L, CAP - former)
    latter = jax.random.randint(keys[1], (pairs,), 2, room + 1)
    chosen = jax.random.randint(keys[2], (), 0, pairs)
    index_pair = jnp.arange(pairs)
    former = jnp.where(index_pair == chosen, L, former)
    latter = jnp.where(index_pair == chosen, CAP - L, latter)
    swapped = jax.random.randint(keys[3], (pairs,), 0, 2)
    head_len = jnp.where(swapped == 1, latter, former)
    tail_len = jnp.where(swapped == 1, former, latter)
    return jnp.stack([head_len, tail_len], axis=1).reshape(DOCS).astype(jnp.int32)


def draw_head_table(key, part):
    keys = jax.random.split(jax.random.fold_in(key, 37), 1)
    base = jnp.clip(jax.random.normal(keys[0], (V, D), jnp.float32), -6.0, 6.0) * (3.0 / math.sqrt(D))
    base = jnp.clip(base, -12.0, 12.0)
    return base.astype(jnp.bfloat16)


def with_ends(values, rng, low, high):
    longest = values.shape.index(max(values.shape))
    spots = []
    for shift in (0, 1):
        where = [jax.random.randint(jax.random.fold_in(rng, axis), (), 0, length) for axis, length in enumerate(values.shape)]
        where[longest] = (where[longest] + shift) % values.shape[longest]
        spots.append(tuple(where))
    return values.at[spots[0]].set(low).at[spots[1]].set(high)


def levels(rng, dims, cuts, low, largest):
    loudness = 1.0
    for axis_at, shards_of in cuts:
        steps = jax.random.uniform(jax.random.fold_in(jax.random.fold_in(rng, 6), axis_at), (shards_of,), jnp.float32, low / len(cuts), largest / len(cuts))
        loudness = loudness * jnp.repeat(jnp.exp(steps), dims[axis_at] // shards_of).reshape((-1,) + (1,) * (len(dims) - 1 - axis_at))
    return loudness


def ranked_wide(own_key, extent, count, lean):
    loads = [min(1 << octave, count + 1 - (1 << octave)) * (1 << 20) // math.isqrt((1 << octave) ** lean) + 1 for octave in range((count + 1).bit_length()) if 1 << octave <= count]
    deviation = 1 + sum(loads) // (1 << 30)
    table = np.cumsum(np.array([max(1, weight // deviation) for weight in loads]))
    ticket = jax.random.randint(jax.random.fold_in(own_key, 1), extent, 0, int(table[len(loads) - 1]))
    start = jnp.left_shift(1, jnp.searchsorted(jnp.asarray(table, jnp.int32), ticket, side="right").astype(jnp.int32))
    rank = start - 1 + jax.random.randint(jax.random.fold_in(own_key, 4), extent, 0, 1 << 30) % jnp.minimum(start, count + 1 - start)
    return jax.random.permutation(jax.random.fold_in(own_key, 2), count)[rank].astype(jnp.int32)


def centred(own_key, extent, width, reach, shards=(), kind=jnp.bfloat16):
    entries = width * jax.random.normal(own_key, extent, jnp.float32)
    if shards:
        entries = entries * levels(own_key, extent, shards, -0.22, 0.18)
    return jnp.clip(entries, -reach, reach).astype(kind)


def setup_inputs(seed: int = 0) -> dict:
    key_of = jax.random.split(jax.random.key(seed), 11)
    return {
        "hidden_in": centred(key_of[0], (DOCS, L, D), 1.0, 6.0, ((0, 256),)),
        "tokens": with_ends(ranked_wide(key_of[1], (DOCS, L), V, 2), jax.random.fold_in(key_of[1], 3), 0, V - 1).astype(jnp.int32),
        "lengths": draw_lengths(jax.random.fold_in(key_of[10], 71), 0),
        "cutoff": jax.random.randint(key_of[3], (1,), 1, DOCS + 1).astype(jnp.int32),
        "norm_gain": jnp.clip(jax.random.uniform(key_of[4], (D,), jnp.float32, 0.5, 1.5), 0.5, 1.5),
        "gate_weight": centred(key_of[5], (D, FF), D ** -0.5, 0.1875, ((1, 4),)),
        "up_weight": centred(key_of[6], (D, FF), D ** -0.5, 0.1875, ((1, 4),)),
        "down_weight": centred(key_of[7], (FF, D), FF ** -0.5, 0.09375, ((0, 4),)),
        "final_gain": jnp.clip(jax.random.uniform(key_of[8], (D,), jnp.float32, 0.5, 1.5), 0.5, 1.5),
        "head_table": draw_head_table(jax.random.fold_in(key_of[10], 71), 0),
    }


def rms_norm(values, gain):
    squares = lax.optimization_barrier(jnp.mean(values * values, axis=-1, keepdims=True))
    return values * lax.rsqrt(squares + 1e-06) * gain

def reference(hidden_in, tokens, lengths, cutoff, norm_gain, gate_weight, up_weight, down_weight, final_gain, head_table):
    residual = hidden_in.reshape(-1, D).astype(jnp.float32)
    normed = rms_norm(residual, norm_gain).astype(jnp.bfloat16)
    gate_part = jnp.dot(normed, gate_weight, preferred_element_type=jnp.float32)
    up_part = jnp.dot(normed, up_weight, preferred_element_type=jnp.float32)
    active = (jax.nn.silu(gate_part) * up_part).astype(jnp.bfloat16)
    stream = (residual + jnp.dot(active, down_weight, preferred_element_type=jnp.float32)).astype(jnp.bfloat16)
    final_rows = rms_norm(stream.astype(jnp.float32), final_gain).astype(jnp.bfloat16)
    targets = jnp.concatenate([tokens[:, 1:], tokens[:, :1]], axis=1).reshape(-1).astype(jnp.int32)
    row_total = final_rows.shape[0]
    block_size = math.gcd(row_total, 256)

    def score_block(block_pair):
        block_part, block_targets = block_pair
        logits = lax.dot_general(block_part, head_table, (((1,), (1,)), ((), ())), preferred_element_type=jnp.float32)
        highest = lax.optimization_barrier(jnp.max(logits, axis=1))
        exp_sum = lax.optimization_barrier(jnp.sum(jnp.exp(logits - highest[:, None]), axis=1))
        picked = jnp.take_along_axis(logits, block_targets[:, None], axis=1)[:, 0]
        return highest + jnp.log(exp_sum) - picked
    nll = lax.map(score_block, (final_rows.reshape(row_total // block_size, block_size, D), targets.reshape(row_total // block_size, block_size)))
    nll = nll.reshape(DOCS, L)
    position = jnp.arange(L, dtype=jnp.int32)
    live_mask = position[None, :] < lengths[:, None] - 1
    log_ppl = lax.optimization_barrier(jnp.sum(jnp.where(live_mask, nll, 0.0), axis=1)) / (lengths - 1).astype(nll.dtype)
    ordered = jnp.sort(log_ppl)
    threshold = lax.dynamic_index_in_dim(ordered, (cutoff[0] - 1).astype(jnp.int32), 0, keepdims=False)
    return (log_ppl, log_ppl - threshold)
```

```python
import functools

import jax
import jax.numpy as jnp
from jax import lax
from jax.experimental import pallas as pl
from jax.experimental.pallas import tpu as pltpu
from jax.sharding import Mesh
from jax.sharding import PartitionSpec as P

CAP = 32
EXTRA = 8
AXES = ("z", "y", "c", "x")
X_STEPS = (0, 1, -1, 2)


def shift(array, axis, step):
    length = lax.axis_size(axis)
    return lax.ppermute(array, axis, [(i, (i + step) % length) for i in range(length)])


def rms_norm(values, gain):
    squares = jnp.mean(values * values, axis=-1, keepdims=True)
    return values * lax.rsqrt(squares + 1e-06) * gain


def score_chunks(chunks, tables, offsets, halves):
    rows_each = 4 * CAP
    count = 1 if halves else len(chunks)
    total = rows_each * count
    width = sum(c.shape[1] for c in chunks) if halves else chunks[0].shape[1]
    tile = 256

    def kernel(offset_ref, *refs):
        chunk_refs = refs[: len(chunks)]
        table_refs = refs[len(chunks) : len(chunks) + len(tables)]
        out_ref, rows, buffers, sems = (
            refs[len(chunks) + len(tables)],
            refs[len(chunks) + len(tables) + 1],
            refs[len(chunks) + len(tables) + 2 : -1],
            refs[-1],
        )
        copies = [
            pltpu.make_async_copy(table_refs[k], buffers[k], sems.at[k])
            for k in range(len(tables))
        ]
        for copy in copies:
            copy.start()
        metas = []
        if halves:
            half = width // 2
            rows[:, :half] = chunk_refs[0][:rows_each, :]
            rows[:, half:] = chunk_refs[1][:rows_each, :]
            metas.append(chunk_refs[0][rows_each:, :rows_each].astype(jnp.float32))
        else:
            for k, ref in enumerate(chunk_refs):
                rows[k * rows_each : (k + 1) * rows_each, :] = ref[:rows_each, :]
                metas.append(ref[rows_each:, :rows_each].astype(jnp.float32))
        target = jnp.concatenate(
            [meta[0:1] + 256.0 * meta[1:2] + 65536.0 * meta[2:3] for meta in metas], axis=1
        ).astype(jnp.int32)
        left = rows[...]
        peak = jnp.full((8, total), -3.0e38, jnp.float32)
        exp_sum = jnp.zeros((8, total), jnp.float32)
        picked = jnp.zeros((8, total), jnp.float32)
        column = lax.broadcasted_iota(jnp.int32, (tile, total), 0)
        for k in range(len(tables)):
            copies[k].wait()
            local = target - offset_ref[k]
            for start in range(0, tables[k].shape[0], tile):
                logits = lax.dot_general(
                    buffers[k][start : start + tile, :],
                    left,
                    (((1,), (1,)), ((), ())),
                    preferred_element_type=jnp.float32,
                )
                found = jnp.where(column == local - start, logits, 0.0)
                grouped = logits.reshape(tile // 8, 8, total)
                highest = jnp.maximum(peak, jnp.max(grouped, axis=0))
                exp_sum = exp_sum * jnp.exp(peak - highest) + jnp.sum(
                    jnp.exp(grouped - highest[None]), axis=0
                )
                picked = picked + jnp.sum(found.reshape(tile // 8, 8, total), axis=0)
                peak = highest
        top = jnp.max(peak, axis=0, keepdims=True)
        total_exp = jnp.sum(exp_sum * jnp.exp(peak - top), axis=0, keepdims=True)
        lse = top + jnp.log(total_exp)
        pick = jnp.sum(picked, axis=0, keepdims=True)
        for k, meta in enumerate(metas):
            part = slice(k * rows_each, (k + 1) * rows_each)
            first = jnp.where(meta[3:4] > 0.0, 1.0 / jnp.maximum(meta[3:4], 1.0), 0.0)
            second = jnp.where(meta[4:5] > 0.0, 1.0 / jnp.maximum(meta[4:5], 1.0), 0.0)
            out_ref[k, 0:1, :] = lse[:, part]
            out_ref[k, 1:2, :] = first * pick[:, part]
            out_ref[k, 2:3, :] = second * pick[:, part]
            out_ref[k, 3:4, :] = first
            out_ref[k, 4:5, :] = second
            out_ref[k, 5:8, :] = jnp.zeros((3, rows_each), jnp.float32)

    table_rows = sum(t.shape[0] for t in tables)
    return pl.pallas_call(
        kernel,
        out_shape=jax.ShapeDtypeStruct((count, 8, rows_each), jnp.float32),
        in_specs=[pl.BlockSpec(memory_space=pltpu.SMEM)]
        + [pl.BlockSpec(memory_space=pltpu.VMEM)] * len(chunks)
        + [pl.BlockSpec(memory_space=pl.ANY)] * len(tables),
        out_specs=pl.BlockSpec(memory_space=pltpu.VMEM),
        scratch_shapes=[pltpu.VMEM((total, width), jnp.bfloat16)]
        + [pltpu.VMEM(t.shape, t.dtype) for t in tables]
        + [pltpu.SemaphoreType.DMA((len(tables),))],
        cost_estimate=pl.CostEstimate(
            flops=2 * total * width * table_rows,
            bytes_accessed=2 * width * table_rows,
            transcendentals=total * table_rows,
        ),
        compiler_params=pltpu.CompilerParams(vmem_limit_bytes=24 * 1024 * 1024),
    )(offsets, *chunks, *tables)


def on_device(
    hidden_in,
    tokens,
    lengths,
    cutoff,
    norm_gain,
    gate_weight,
    up_weight,
    down_weight,
    final_gain,
    head_table,
):
    doc_count, length, width = hidden_in.shape
    shard = head_table.shape[0]
    here = {axis: lax.axis_index(axis) for axis in AXES}
    size = {axis: lax.axis_size(axis) for axis in AXES}

    half_shard = shard // 2
    other_core = shift(head_table, "c", 1)
    from_below = shift(head_table, "y", 1)
    from_above = shift(head_table, "y", -1)

    live = lengths - 1
    slot = jnp.arange(CAP, dtype=jnp.int32)
    in_first = slot < live[0]
    in_second = (slot >= live[0]) & (slot < live[0] + live[1])
    source = jnp.where(in_first, slot, length + slot - live[0])
    position = jnp.arange(doc_count * length, dtype=jnp.int32)
    used = in_first | in_second
    placing = (source[:, None] == position[None, :]) & used[:, None]
    residual = jnp.dot(
        placing.astype(jnp.bfloat16),
        hidden_in.reshape(doc_count * length, width),
        preferred_element_type=jnp.float32,
    )
    next_place = (source[:, None] + 1 == position[None, :]) & used[:, None]
    targets = jnp.sum(
        jnp.where(next_place, tokens.reshape(doc_count * length)[None, :], 0), axis=1
    )
    extra = jnp.stack(
        [
            targets & 255,
            (targets >> 8) & 255,
            targets >> 16,
            jnp.where(in_first, live[0], 0),
            jnp.where(in_second, live[1], 0),
        ]
    ).astype(jnp.bfloat16)
    extra = jnp.pad(extra, ((0, EXTRA - extra.shape[0]), (0, width - CAP)))

    normed = rms_norm(residual, norm_gain).astype(jnp.bfloat16)
    sent = jnp.concatenate([normed, extra])
    arrived = [sent if step == 0 else shift(sent, "x", step) for step in X_STEPS]
    segment = jnp.concatenate([part[:CAP] for part in arrived])
    meta = jnp.concatenate([part[CAP:, :CAP] for part in arrived], axis=1)
    meta = jnp.pad(meta, ((0, 0), (0, width - meta.shape[1])))

    gate_part = jnp.dot(segment, gate_weight, preferred_element_type=jnp.float32)
    up_part = jnp.dot(segment, up_weight, preferred_element_type=jnp.float32)
    active = (jax.nn.silu(gate_part) * up_part).astype(jnp.bfloat16)
    partial = jnp.dot(active, down_weight, preferred_element_type=jnp.float32)
    branch = partial[:CAP]
    for k, step in enumerate(X_STEPS):
        if step != 0:
            part = partial[k * CAP : (k + 1) * CAP].astype(jnp.bfloat16)
            branch = branch + shift(part, "x", -step).astype(jnp.float32)
    stream = (residual + branch).astype(jnp.bfloat16)
    final_rows = rms_norm(stream.astype(jnp.float32), final_gain).astype(jnp.bfloat16)

    final_rows, from_below, from_above, other_core = lax.optimization_barrier(
        (final_rows, from_below, from_above, other_core)
    )
    chunk = jnp.concatenate(
        [final_rows if step == 0 else shift(final_rows, "x", step) for step in X_STEPS] + [meta]
    )
    far_low = shift(from_below[:half_shard], "y", 1)
    far_high = shift(from_above[half_shard:], "y", -1)
    below_other = shift(from_below, "c", 1)
    above_other = shift(from_above, "c", 1)

    up_1, down_1 = shift(chunk, "z", 1), shift(chunk, "z", -1)
    up_1, down_1, far_low, far_high = lax.optimization_barrier((up_1, down_1, far_low, far_high))
    up_2, down_2 = shift(up_1, "z", 1), shift(down_1, "z", -1)
    far_low_other = shift(far_low, "c", 1)
    far_high_other = shift(far_high, "c", 1)
    up_3, down_3 = shift(up_2, "z", 1), shift(down_2, "z", -1)
    half = width // 2
    across = (shift(up_3[:, :half], "z", 1), shift(down_3[:, half:], "z", -1))

    def first_row(y_step, c_step, begin=0):
        y_at = (here["y"] + y_step) % size["y"]
        c_at = (here["c"] + c_step) % size["c"]
        at = ((here["z"] * size["y"] + y_at) * size["c"] + c_at) * size["x"] + here["x"]
        return at * shard + begin

    tables = [
        (head_table, first_row(0, 0)),
        (other_core, first_row(0, 1)),
        (from_below, first_row(-1, 0)),
        (from_above, first_row(1, 0)),
        (below_other, first_row(-1, 1)),
        (above_other, first_row(1, 1)),
        (far_low, first_row(2, 0)),
        (far_high, first_row(2, 0, half_shard)),
        (far_low_other, first_row(2, 1)),
        (far_high_other, first_row(2, 1, half_shard)),
    ]
    offsets = jnp.stack([offset for _, offset in tables]).astype(jnp.int32)
    tables = [table for table, _ in tables]
    score = functools.partial(score_chunks, tables=tables, offsets=offsets)
    own = score([chunk], halves=False)
    near = score([up_1, down_1], halves=False)
    middle = score([up_2, down_2], halves=False)
    outer = score([up_3, down_3], halves=False)
    last = score(list(across), halves=True)
    found = jnp.stack(
        [own[0], near[1], middle[1], outer[1], last[0], outer[0], middle[0], near[0]]
    )
    z_order = (
        (jnp.arange(size["z"])[:, None] - here["z"]) % size["z"] == jnp.arange(size["z"])[None, :]
    ).astype(jnp.float32)
    lane = jnp.arange(4 * CAP, dtype=jnp.int32)
    sources = jnp.array([0, -1, 1, 2], jnp.int32)
    source_x = (here["x"] + jnp.repeat(sources, CAP)) % size["x"]
    x_order = ((source_x * CAP + lane % CAP)[:, None] == lane[None, :]).astype(jnp.float32)
    flat = found.reshape(size["z"], 8 * 4 * CAP)
    flat = jnp.dot(z_order, flat, precision=lax.Precision.HIGHEST)
    placed = jnp.dot(
        flat.reshape(size["z"] * 8, 4 * CAP), x_order, precision=lax.Precision.HIGHEST
    ).reshape(size["z"], 8, 4 * CAP)
    lse, pick_first, pick_second = placed[:, 0], placed[:, 1], placed[:, 2]
    weight_first, weight_second = placed[:, 3], placed[:, 4]

    def per_device(values):
        return jnp.sum(values.reshape(size["z"], size["x"], CAP), axis=2)

    picks = jnp.stack([per_device(pick_first), per_device(pick_second)], axis=2)
    picks = jnp.pad(picks.reshape(1, -1), ((0, 0), (0, 4 * CAP - 2 * size["z"] * size["x"])))
    message = jnp.concatenate([lse, picks])
    members = size["z"] * size["x"]
    everyone = lax.all_to_all(
        jnp.broadcast_to(message[None], (members, *message.shape)), ("z", "x"), 0, 0, tiled=True
    )
    parts = everyone[:, : size["z"]]
    top = jnp.max(parts, axis=0)
    lse = top + jnp.log(jnp.sum(jnp.exp(parts - top[None]), axis=0))
    picks = jnp.sum(everyone[:, size["z"]], axis=0)[: 2 * members].reshape(size["z"], size["x"], 2)
    group = (
        jnp.stack([per_device(lse * weight_first), per_device(lse * weight_second)], axis=2)
        - picks
    )
    mine = (
        (jnp.arange(size["z"])[:, None] == here["z"])
        & (jnp.arange(size["x"])[None, :] == here["x"])
    )[:, :, None]
    log_ppl = jnp.sum(jnp.where(mine, group, 0.0), axis=(0, 1))
    line = group.reshape(1, 2 * members)
    pair = jnp.concatenate([line, shift(line, "c", 1)], axis=1)
    values = jnp.concatenate(
        [pair, shift(pair, "y", 1), shift(pair, "y", -1), shift(pair, "y", 2)], axis=0
    ).reshape(-1)
    not_above = jnp.sum((values[None, :] <= values[:, None]).astype(jnp.int32), axis=1)
    threshold = jnp.min(jnp.where(not_above >= cutoff[0], values, jnp.inf))
    return (log_ppl, log_ppl - threshold)


def solution(mesh):
    finer = Mesh(mesh.devices.reshape(8, 4, 2, mesh.shape["vocab"]), AXES)
    return jax.shard_map(
        on_device,
        mesh=finer,
        in_specs=(
            P(AXES, None, None),
            P(AXES, None),
            P(AXES),
            P(),
            P(),
            P(None, "x"),
            P(None, "x"),
            P("x", None),
            P(),
            P(AXES, None),
        ),
        out_specs=(P(AXES), P(AXES)),
        check_vma=False,
    )
```

```python
import jax
import jax.numpy as jnp
from jax import lax
from jax.experimental import pallas as pl
from jax.experimental.pallas import tpu as pltpu
from jax.sharding import Mesh
from jax.sharding import PartitionSpec as P

CAP = 32
EXTRA = 8
LANES = 4 * CAP
TILE = 256
AXES = ("z", "y", "c", "x")
X_STEPS = (0, -1, 2, 1)
HIGHEST = lax.Precision.HIGHEST
F32 = jnp.float32
BF16 = jnp.bfloat16
VMEM = pl.BlockSpec(memory_space=pltpu.VMEM)
SMEM = pl.BlockSpec(memory_space=pltpu.SMEM)


def params(mib):
    return pltpu.CompilerParams(vmem_limit_bytes=mib * 1024 * 1024)


def cost(flops, moved=0, exps=0):
    return pl.CostEstimate(flops=flops, bytes_accessed=moved, transcendentals=exps)


def shift(array, axis, step):
    length = lax.axis_size(axis)
    return lax.ppermute(array, axis, [(i, (i + step) % length) for i in range(length)])


def rms_norm(values, gain):
    squares = jnp.mean(values * values, axis=-1, keepdims=True)
    return values * lax.rsqrt(squares + 1e-06) * gain


def iota(shape, dim):
    return lax.broadcasted_iota(jnp.int32, shape, dim)


def prepare_kernel(lengths_ref, tokens_ref, hidden_ref, gain_ref, sent_ref, residual_ref):
    docs, length, width = hidden_ref.shape
    lives = [lengths_ref[d] - 1 for d in range(docs)]
    starts = [0, lives[0]]
    residual = jnp.zeros((CAP, width), F32)
    target = jnp.zeros((8, CAP), F32)
    slot_down, place_right = iota((CAP, length), 0), iota((CAP, length), 1)
    place_down, slot_right = iota((length, CAP), 0), iota((length, CAP), 1)
    for d in range(docs):
        live = (slot_down >= starts[d]) & (slot_down < starts[d] + lives[d])
        placing = (place_right == slot_down - starts[d]) & live
        residual = residual + jnp.dot(
            placing.astype(BF16), hidden_ref[d], preferred_element_type=F32
        )
        live = (slot_right >= starts[d]) & (slot_right < starts[d] + lives[d])
        taking = (place_down == slot_right - starts[d] + 1) & live
        token = tokens_ref[d : d + 1, :]
        digits = [token & 255, (token >> 8) & 255, token >> 16]
        digits = jnp.concatenate(digits + [jnp.zeros((5, length), jnp.int32)], axis=0)
        target = target + jnp.dot(
            digits.astype(F32).astype(BF16), taking.astype(BF16), preferred_element_type=F32
        )
    residual_ref[...] = residual.astype(BF16)
    sent_ref[:CAP, :] = rms_norm(residual, gain_ref[...]).astype(BF16)
    row, slot = iota((8, CAP), 0), iota((8, CAP), 1)
    for d in range(docs):
        live = (slot >= starts[d]) & (slot < starts[d] + lives[d]) & (row == 3 + d)
        target = jnp.where(live, lives[d].astype(F32), target)
    sent_ref[CAP:, :] = jnp.concatenate([target, jnp.zeros((8, width - CAP), F32)], axis=1).astype(
        BF16
    )


def feed_kernel(*refs):
    arrived, (gate_ref, up_ref, down_ref) = refs[:4], refs[4:7]
    own_ref, out_refs, meta_ref, rows = refs[7], refs[8:11], refs[11], refs[12]
    for k, ref in enumerate(arrived):
        rows[k * CAP : (k + 1) * CAP, :] = ref[:CAP, :]
    metas = jnp.concatenate([ref[CAP:, :CAP].astype(F32) for ref in arrived], axis=1)
    meta_ref[...] = jnp.zeros_like(meta_ref)
    meta_ref[:, :LANES] = metas.astype(BF16)
    segment = rows[...]
    units = gate_ref.shape[1]
    total = jnp.zeros((4 * CAP, down_ref.shape[1]), F32)
    for at in range(0, units, TILE):
        gate = jnp.dot(segment, gate_ref[:, at : at + TILE], preferred_element_type=F32)
        up = jnp.dot(segment, up_ref[:, at : at + TILE], preferred_element_type=F32)
        active = (gate / (1.0 + jnp.exp(-gate)) * up).astype(BF16)
        total = total + jnp.dot(
            active, down_ref[at : at + TILE, :], preferred_element_type=F32
        )
    own_ref[...] = total[:CAP]
    for k, ref in enumerate(out_refs):
        ref[...] = total[(k + 1) * CAP : (k + 2) * CAP].astype(BF16)


def finish_kernel(own_ref, first_ref, second_ref, third_ref, residual_ref, gain_ref, out_ref):
    branch = own_ref[...] + first_ref[...].astype(F32)
    branch = branch + second_ref[...].astype(F32) + third_ref[...].astype(F32)
    stream = (residual_ref[...].astype(F32) + branch).astype(BF16)
    out_ref[...] = rms_norm(stream.astype(F32), gain_ref[...]).astype(BF16)


def join_kernel(*refs):
    out_ref, at = refs[-1], 0
    for ref in refs[:-1]:
        out_ref[at : at + ref.shape[0], :] = ref[...]
        at += ref.shape[0]


def score_kernel(halves, table_steps, *refs):
    chunk_refs, refs = refs[: 3 if halves else 2], refs[3 if halves else 2 :]
    table_refs, (out_ref, rows) = refs[:-2], refs[-2:]
    half = rows.shape[1] // 2
    rows[:LANES, :] = chunk_refs[0][:LANES, :]
    if halves:
        rows[LANES:, :half] = chunk_refs[1][:LANES, :]
        rows[LANES:, half:] = chunk_refs[2][:LANES, :]
    else:
        rows[LANES:, :] = chunk_refs[1][:LANES, :]
    metas = [ref[LANES:, :LANES].astype(F32) for ref in chunk_refs[:2]]
    target = jnp.concatenate(
        [meta[0:1] + 256.0 * meta[1:2] + 65536.0 * meta[2:3] for meta in metas], axis=1
    ).astype(jnp.int32)
    total = 2 * LANES
    left = rows[...]
    peak = jnp.full((8, total), -3.0e38, F32)
    exp_sum = jnp.zeros((8, total), F32)
    picked = jnp.zeros((8, total), F32)
    column = iota((TILE, total), 0)
    z, y, c, x = [lax.axis_index(axis) for axis in AXES]
    for table, (y_step, c_step, begin) in zip(table_refs, table_steps):
        shard_at = ((z * 4 + lax.rem(y + y_step, 4)) * 2 + lax.rem(c + c_step, 2)) * 4 + x
        local = target - (shard_at * (2 * TILE) + begin)
        for start in range(0, table.shape[0], TILE):
            logits = lax.dot_general(
                table[start : start + TILE, :],
                left,
                (((1,), (1,)), ((), ())),
                preferred_element_type=F32,
            )
            found = jnp.where(column == local - start, logits, 0.0)
            grouped = logits.reshape(TILE // 8, 8, total)
            highest = jnp.maximum(peak, jnp.max(grouped, axis=0))
            exp_sum = exp_sum * jnp.exp(peak - highest) + jnp.sum(
                jnp.exp(grouped - highest[None]), axis=0
            )
            picked = picked + jnp.sum(found.reshape(TILE // 8, 8, total), axis=0)
            peak = highest
    top = jnp.max(peak, axis=0, keepdims=True)
    lse = top + jnp.log(jnp.sum(exp_sum * jnp.exp(peak - top), axis=0, keepdims=True))
    pick = jnp.sum(picked, axis=0, keepdims=True)
    for k, meta in enumerate(metas):
        part = slice(k * LANES, (k + 1) * LANES)
        first, second = [
            jnp.where(line > 0.0, 1.0 / jnp.maximum(line, 1.0), 0.0)
            for line in (meta[3:4], meta[4:5])
        ]
        lines = [lse[:, part], first * pick[:, part], second * pick[:, part], first, second]
        out_ref[k] = jnp.concatenate(lines + [jnp.zeros((3, LANES), F32)], axis=0)


def document_sums(first, second):
    slot_at, lane_at = iota((LANES, LANES), 0), iota((LANES, LANES), 1)
    same = slot_at // CAP == lane_at // CAP
    sums = jnp.zeros_like(first)
    for values, lane in ((first, CAP - 2), (second, CAP - 1)):
        into = (same & (lane_at % CAP == lane)).astype(F32)
        sums = sums + jnp.dot(values, into, precision=HIGHEST, preferred_element_type=F32)
    return sums


def message_kernel(near_ref, middle_ref, outer_ref, last_ref, out_ref, weight_ref):
    order = [
        last_ref[0],
        near_ref[1],
        middle_ref[1],
        outer_ref[1],
        last_ref[1],
        outer_ref[0],
        middle_ref[0],
        near_ref[0],
    ]
    kinds = [jnp.concatenate([part[k : k + 1] for part in order], axis=0) for k in range(5)]
    kinds = [
        pltpu.roll(pltpu.roll(kind, lax.axis_index("z"), 0), lax.axis_index("x") * CAP, 1)
        for kind in kinds
    ]
    lse, pick_first, pick_second, weight_first, weight_second = kinds
    weight_ref[0] = weight_first
    weight_ref[1] = weight_second
    carried = iota((8, LANES), 1) % CAP >= CAP - 2
    message = jnp.where(carried, document_sums(pick_first, pick_second), lse)
    for k in range(out_ref.shape[0]):
        out_ref[k] = message


def merge_kernel(everyone_ref, weight_ref, out_ref):
    members = everyone_ref.shape[0]
    top = everyone_ref[0]
    total = everyone_ref[0]
    for k in range(1, members):
        top = jnp.maximum(top, everyone_ref[k])
        total = total + everyone_ref[k]
    exp_sum = jnp.zeros_like(top)
    for k in range(members):
        exp_sum = exp_sum + jnp.exp(everyone_ref[k] - top)
    lse = top + jnp.log(exp_sum)
    carried = iota((8, LANES), 1) % CAP >= CAP - 2
    lse = jnp.where(carried, 0.0, lse)
    sums = document_sums(weight_ref[0] * lse, weight_ref[1] * lse)
    out_ref[...] = jnp.where(carried, sums - total, 0.0)


def select_kernel(cutoff_ref, *refs):
    parts, (log_ref, margin_ref) = refs[:4], refs[4:6]
    values = jnp.concatenate([part[...] for part in parts], axis=0)
    across = values.T
    count = values.shape[0]
    lanes = [x * CAP + CAP - 2 + d for x in range(4) for d in range(2)]
    best = jnp.full((count, 1), jnp.inf, F32)
    for lane in lanes:
        value = values[:, lane : lane + 1]
        below = jnp.zeros((count, count), F32)
        for other in lanes:
            below = below + jnp.where(across[other : other + 1, :] <= value, 1.0, 0.0)
        rank = jnp.sum(below, axis=1, keepdims=True)
        best = jnp.minimum(
            best, jnp.where(rank >= cutoff_ref[0].astype(F32), value, jnp.inf)
        )
    threshold = jnp.min(best)
    own = values[:8]
    row, lane_at = iota((8, LANES), 0), iota((8, LANES), 1)
    for d in range(2):
        here = (row == lax.axis_index("z")) & (
            lane_at == lax.axis_index("x") * CAP + CAP - 2 + d
        )
        log_ppl = jnp.sum(jnp.where(here, own, 0.0))
        log_ref[d] = log_ppl
        margin_ref[d] = log_ppl - threshold


def on_device(
    hidden_in,
    tokens,
    lengths,
    cutoff,
    norm_gain,
    gate_weight,
    up_weight,
    down_weight,
    final_gain,
    head_table,
):
    width = hidden_in.shape[2]
    shard = head_table.shape[0]
    half_shard, half = shard // 2, width // 2
    size = {axis: lax.axis_size(axis) for axis in AXES}

    sent, residual = pl.pallas_call(
        prepare_kernel,
        out_shape=(
            jax.ShapeDtypeStruct((CAP + EXTRA, width), BF16),
            jax.ShapeDtypeStruct((CAP, width), BF16),
        ),
        in_specs=[SMEM, VMEM, VMEM, VMEM],
        out_specs=(VMEM, VMEM),
        cost_estimate=cost(4_000_000),
        compiler_params=params(4),
    )(lengths, tokens, hidden_in, norm_gain.reshape(1, width))
    arrived = [sent if step == 0 else shift(sent, "x", step) for step in X_STEPS]

    low, high = head_table[:half_shard], head_table[half_shard:]
    below_low, above_high = shift(low, "y", 1), shift(high, "y", -1)
    below_high, above_low = shift(high, "y", 1), shift(low, "y", -1)
    other_core = shift(head_table, "c", 1)

    partials = pl.pallas_call(
        feed_kernel,
        out_shape=(
            jax.ShapeDtypeStruct((CAP, width), F32),
            *(jax.ShapeDtypeStruct((CAP, width), BF16),) * 3,
            jax.ShapeDtypeStruct((EXTRA, width), BF16),
        ),
        in_specs=[VMEM] * 7,
        out_specs=(VMEM,) * 5,
        scratch_shapes=[pltpu.VMEM((4 * CAP, width), BF16)],
        cost_estimate=cost(800_000_000, 6_300_000, 131072),
        compiler_params=params(16),
    )(*arrived, gate_weight, up_weight, down_weight)
    own_part, parts, meta = partials[0], partials[1:4], partials[4]
    returned = [shift(part, "x", -step) for part, step in zip(parts, X_STEPS[1:])]
    final_rows = pl.pallas_call(
        finish_kernel,
        out_shape=jax.ShapeDtypeStruct((CAP, width), BF16),
        in_specs=[VMEM] * 6,
        out_specs=VMEM,
        cost_estimate=cost(1_000_000),
        compiler_params=params(4),
    )(own_part, *returned, residual, final_gain.reshape(1, width))

    final_rows, below_low, above_high = lax.optimization_barrier(
        (final_rows, below_low, above_high)
    )
    far_low, far_high = shift(below_low, "y", 1), shift(above_high, "y", -1)
    chunk = pl.pallas_call(
        join_kernel,
        out_shape=jax.ShapeDtypeStruct((LANES + EXTRA, width), BF16),
        in_specs=[VMEM] * 5,
        out_specs=VMEM,
        cost_estimate=cost(500_000),
        compiler_params=params(4),
    )(*[final_rows if step == 0 else shift(final_rows, "x", step) for step in X_STEPS], meta)

    up_1, down_1 = shift(chunk, "z", 1), shift(chunk, "z", -1)
    chunk, below_high, above_low, below_low, above_high = lax.optimization_barrier(
        (chunk, below_high, above_low, below_low, above_high)
    )
    near_halves = [below_low, below_high, above_low, above_high]
    near_other = [shift(part, "c", 1) for part in near_halves]
    up_1, down_1, far_low, far_high = lax.optimization_barrier((up_1, down_1, far_low, far_high))
    far_other = [shift(part, "c", 1) for part in (far_low, far_high)]
    up_2, down_2 = shift(up_1, "z", 1), shift(down_1, "z", -1)

    near_steps = ((3, 0), (3, half_shard), (1, 0), (1, half_shard))
    far_steps = ((2, 0), (2, half_shard))
    tables = [head_table, other_core, *near_halves, *near_other, far_low, far_high, *far_other]
    table_steps = [(0, 0, 0), (0, 1, 0)]
    for steps in (near_steps, far_steps):
        table_steps += [(y_step, core, begin) for core in range(2) for y_step, begin in steps]

    def score(chunks):
        rows = 2 * LANES
        halves = len(chunks) == 3

        def kernel(*refs):
            score_kernel(halves, table_steps, *refs)

        return pl.pallas_call(
            kernel,
            out_shape=jax.ShapeDtypeStruct((2, 8, LANES), F32),
            in_specs=[VMEM] * (len(chunks) + len(tables)),
            out_specs=VMEM,
            scratch_shapes=[pltpu.VMEM((rows, width), BF16)],
            cost_estimate=cost(2 * rows * width * 8 * shard, 2 * width * 8 * shard, rows * 8 * shard),
            compiler_params=params(24),
        )(*chunks, *tables)

    near = score([up_1, down_1])
    up_2, down_2, near = lax.optimization_barrier((up_2, down_2, near))
    up_3, down_3 = shift(up_2, "z", 1), shift(down_2, "z", -1)
    middle = score([up_2, down_2])
    up_3, down_3, middle = lax.optimization_barrier((up_3, down_3, middle))
    across = (shift(up_3[:, :half], "z", 1), shift(down_3[:, half:], "z", -1))
    outer = score([up_3, down_3])
    *across, outer = lax.optimization_barrier((*across, outer))
    last = score([chunk, *across])

    members = size["z"] * size["x"]
    message, weights = pl.pallas_call(
        message_kernel,
        out_shape=(
            jax.ShapeDtypeStruct((members, 8, LANES), F32),
            jax.ShapeDtypeStruct((2, 8, LANES), F32),
        ),
        in_specs=[VMEM] * 4,
        out_specs=(VMEM, VMEM),
        cost_estimate=cost(1_000_000),
        compiler_params=params(4),
    )(near, middle, outer, last)
    everyone = lax.all_to_all(message, ("z", "x"), 0, 0, tiled=True)
    group = pl.pallas_call(
        merge_kernel,
        out_shape=jax.ShapeDtypeStruct((8, LANES), F32),
        in_specs=[VMEM, VMEM],
        out_specs=VMEM,
        cost_estimate=cost(1_000_000),
        compiler_params=params(4),
    )(everyone, weights)
    pair = jnp.concatenate([group, shift(group, "c", 1)], axis=0)
    log_ppl, margin = pl.pallas_call(
        select_kernel,
        out_shape=(jax.ShapeDtypeStruct((2,), F32), jax.ShapeDtypeStruct((2,), F32)),
        in_specs=[SMEM] + [VMEM] * 4,
        out_specs=(SMEM, SMEM),
        cost_estimate=cost(1_000_000),
        compiler_params=params(4),
    )(cutoff, pair, shift(pair, "y", 1), shift(pair, "y", -1), shift(pair, "y", 2))
    return (log_ppl, margin)


def solution(mesh):
    finer = Mesh(mesh.devices.reshape(8, 4, 2, mesh.shape["vocab"]), AXES)
    return jax.shard_map(
        on_device,
        mesh=finer,
        in_specs=(
            P(AXES, None, None),
            P(AXES, None),
            P(AXES),
            P(),
            P(),
            P(None, "x"),
            P(None, "x"),
            P("x", None),
            P(),
            P(AXES, None),
        ),
        out_specs=(P(AXES), P(AXES)),
        check_vma=False,
    )
```

```python
import jax
import jax.numpy as jnp
from jax import lax
from jax.experimental import pallas as pl
from jax.experimental.pallas import tpu as pltpu
from jax.sharding import Mesh
from jax.sharding import PartitionSpec as P

CAP = 32
EXTRA = 8
LANES = 4 * CAP
TILE = 256
AXES = ("z", "y", "c", "x")
X_STEPS = (0, -1, 2, 1)
HIGHEST = lax.Precision.HIGHEST
F32 = jnp.float32
BF16 = jnp.bfloat16
VMEM = pl.BlockSpec(memory_space=pltpu.VMEM)
SMEM = pl.BlockSpec(memory_space=pltpu.SMEM)


def params(mib):
    return pltpu.CompilerParams(vmem_limit_bytes=mib * 1024 * 1024)


def cost(flops, moved=0, exps=0):
    return pl.CostEstimate(flops=flops, bytes_accessed=moved, transcendentals=exps)


def shift(array, axis, step):
    length = lax.axis_size(axis)
    pairs = [(i, (i + step) % length) for i in range(length)]
    return lax.ppermute(array, axis, pairs)


def rms_norm(values, gain):
    squares = jnp.mean(values * values, axis=-1, keepdims=True)
    return values * lax.rsqrt(squares + 1e-06) * gain


def iota(shape, dim):
    return lax.broadcasted_iota(jnp.int32, shape, dim)


def prepare_kernel(lengths_ref, tokens_ref, hidden_ref, gain_ref, sent_ref, residual_ref):
    docs, length, width = hidden_ref.shape
    lives = [lengths_ref[d] - 1 for d in range(docs)]
    starts = [0, lives[0]]
    residual = jnp.zeros((CAP, width), F32)
    target = jnp.zeros((8, CAP), F32)
    slot_down, place_right = iota((CAP, length), 0), iota((CAP, length), 1)
    place_down, slot_right = iota((length, CAP), 0), iota((length, CAP), 1)
    for d in range(docs):
        live = (slot_down >= starts[d]) & (slot_down < starts[d] + lives[d])
        placing = (place_right == slot_down - starts[d]) & live
        residual = residual + jnp.dot(
            placing.astype(BF16), hidden_ref[d], preferred_element_type=F32
        )
        live = (slot_right >= starts[d]) & (slot_right < starts[d] + lives[d])
        taking = (place_down == slot_right - starts[d] + 1) & live
        token = tokens_ref[d : d + 1, :]
        digits = [token & 255, (token >> 8) & 255, token >> 16]
        digits = jnp.concatenate(digits + [jnp.zeros((5, length), jnp.int32)], axis=0)
        target = target + jnp.dot(
            digits.astype(F32).astype(BF16), taking.astype(BF16), preferred_element_type=F32
        )
    residual_ref[...] = residual.astype(BF16)
    sent_ref[:CAP, :] = rms_norm(residual, gain_ref[...]).astype(BF16)
    row, slot = iota((8, CAP), 0), iota((8, CAP), 1)
    for d in range(docs):
        live = (slot >= starts[d]) & (slot < starts[d] + lives[d]) & (row == 3 + d)
        target = jnp.where(live, lives[d].astype(F32), target)
    sent_ref[CAP:, :] = jnp.concatenate([target, jnp.zeros((8, width - CAP), F32)], axis=1).astype(
        BF16
    )


def feed_kernel(*refs):
    arrived, (gate_ref, up_ref, down_ref) = refs[:4], refs[4:7]
    own_ref, out_refs, meta_ref, rows = refs[7], refs[8:11], refs[11], refs[12]
    for k, ref in enumerate(arrived):
        rows[k * CAP : (k + 1) * CAP, :] = ref[:CAP, :]
    metas = jnp.concatenate([ref[CAP:, :CAP].astype(F32) for ref in arrived], axis=1)
    meta_ref[...] = jnp.zeros_like(meta_ref)
    meta_ref[:, :LANES] = metas.astype(BF16)
    segment = rows[...]
    units = gate_ref.shape[1]
    total = jnp.zeros((4 * CAP, down_ref.shape[1]), F32)
    for at in range(0, units, 2 * TILE):
        span = slice(at, at + 2 * TILE)
        gate = jnp.dot(segment, gate_ref[:, span], preferred_element_type=F32)
        up = jnp.dot(segment, up_ref[:, span], preferred_element_type=F32)
        active = (gate / (1.0 + jnp.exp(-gate)) * up).astype(BF16)
        total = total + jnp.dot(active, down_ref[span, :], preferred_element_type=F32)
    own_ref[...] = total[:CAP]
    for k, ref in enumerate(out_refs):
        ref[...] = total[(k + 1) * CAP : (k + 2) * CAP].astype(BF16)


def finish_kernel(own_ref, first_ref, second_ref, third_ref, residual_ref, gain_ref, out_ref):
    branch = own_ref[...] + first_ref[...].astype(F32)
    branch = branch + second_ref[...].astype(F32) + third_ref[...].astype(F32)
    stream = (residual_ref[...].astype(F32) + branch).astype(BF16)
    out_ref[...] = rms_norm(stream.astype(F32), gain_ref[...]).astype(BF16)


def join_kernel(*refs):
    out_ref, at = refs[-1], 0
    for ref in refs[:-1]:
        out_ref[at : at + ref.shape[0], :] = ref[...]
        at += ref.shape[0]


def stage_kernel(*refs):
    count = (len(refs) - 1) // 2
    copies = [
        pltpu.make_async_copy(refs[k], refs[count + k], refs[-1].at[k]) for k in range(count)
    ]
    for copy in copies:
        copy.start()
    for copy in copies:
        copy.wait()


def score_kernel(layout, table_steps, *refs):
    chunk_count, held = len(layout), sum(layout)
    chunk_refs, refs = list(refs[:held]), refs[held:]
    table_refs, (out_ref, rows, targets, results) = refs[:-4], refs[-4:]
    metas = []
    for k, parts in enumerate(layout):
        metas.append(chunk_refs[0][LANES:, :LANES].astype(F32))
        span = rows.shape[1] // parts
        for part in range(parts):
            rows[k * LANES : (k + 1) * LANES, part * span : (part + 1) * span] = chunk_refs.pop(0)[
                :LANES, :
            ]
    groups, total = chunk_count // 2, 2 * LANES
    for k, meta in enumerate(metas):
        target = meta[0:1] + 256.0 * meta[1:2] + 65536.0 * meta[2:3]
        targets[k // 2, :, (k % 2) * LANES : (k % 2 + 1) * LANES] = target.astype(jnp.int32)
    column = iota((TILE, total), 0)
    z, y, c, x = [lax.axis_index(axis) for axis in AXES]

    def score_group(group, carry):
        left = rows[pl.ds(pl.multiple_of(group * total, total), total), :]
        target = targets[group]
        peak = jnp.full((8, total), -3.0e38, F32)
        exp_sum = jnp.zeros((8, total), F32)
        picked = jnp.zeros((8, total), F32)
        for table, (y_steps, c_step) in zip(table_refs, table_steps):
            for tile in range(table.shape[0] // TILE):
                y_at, c_at = lax.rem(y + y_steps[tile // 2], 4), lax.rem(c + c_step, 2)
                shard_at = ((z * 4 + y_at) * 2 + c_at) * 4 + x
                local = target - (2 * shard_at + tile % 2) * TILE
                logits = lax.dot_general(
                    table[tile * TILE : (tile + 1) * TILE, :],
                    left,
                    (((1,), (1,)), ((), ())),
                    preferred_element_type=F32,
                )
                found = jnp.where(column == local, logits, 0.0)
                grouped = logits.reshape(TILE // 8, 8, total)
                highest = jnp.maximum(peak, jnp.max(grouped, axis=0))
                exp_sum = exp_sum * jnp.exp(peak - highest) + jnp.sum(
                    jnp.exp(grouped - highest[None]), axis=0
                )
                picked = picked + jnp.sum(found.reshape(TILE // 8, 8, total), axis=0)
                peak = highest
        top = jnp.max(peak, axis=0, keepdims=True)
        lse = top + jnp.log(jnp.sum(exp_sum * jnp.exp(peak - top), axis=0, keepdims=True))
        results[group, 0:1, :] = lse
        results[group, 1:2, :] = jnp.sum(picked, axis=0, keepdims=True)
        return carry

    if groups == 1:
        score_group(0, 0)
    else:
        lax.fori_loop(0, groups, score_group, 0)
    for k, meta in enumerate(metas):
        part = slice((k % 2) * LANES, (k % 2 + 1) * LANES)
        lse, pick = results[k // 2, 0:1, part], results[k // 2, 1:2, part]
        first, second = [
            jnp.where(line > 0.0, 1.0 / jnp.maximum(line, 1.0), 0.0)
            for line in (meta[3:4], meta[4:5])
        ]
        lines = [lse, first * pick, second * pick, first, second]
        out_ref[k] = jnp.concatenate(lines + [jnp.zeros((3, LANES), F32)], axis=0)


def document_sums(first, second):
    slot_at, lane_at = iota((LANES, LANES), 0), iota((LANES, LANES), 1)
    same = slot_at // CAP == lane_at // CAP
    sums = jnp.zeros_like(first)
    for values, lane in ((first, CAP - 2), (second, CAP - 1)):
        into = (same & (lane_at % CAP == lane)).astype(F32)
        sums = sums + jnp.dot(values, into, precision=HIGHEST, preferred_element_type=F32)
    return sums


def message_kernel(near_ref, middle_ref, far_ref, outer_ref, last_ref, out_ref, weight_ref):
    def joined(left, right):
        top = jnp.maximum(left[0:1], right[0:1])
        lse = top + jnp.log(jnp.exp(left[0:1] - top) + jnp.exp(right[0:1] - top))
        return jnp.concatenate([lse, left[1:3] + right[1:3], left[3:]], axis=0)

    near = [joined(near_ref[k], far_ref[k]) for k in range(2)]
    middle = [joined(middle_ref[k], far_ref[2 + k]) for k in range(2)]
    order = [
        last_ref[0],
        near[1],
        middle[1],
        outer_ref[1],
        last_ref[1],
        outer_ref[0],
        middle[0],
        near[0],
    ]
    kinds = [jnp.concatenate([part[k : k + 1] for part in order], axis=0) for k in range(5)]
    kinds = [
        pltpu.roll(pltpu.roll(kind, lax.axis_index("z"), 0), lax.axis_index("x") * CAP, 1)
        for kind in kinds
    ]
    lse, pick_first, pick_second, weight_first, weight_second = kinds
    weight_ref[0] = weight_first
    weight_ref[1] = weight_second
    carried = iota((8, LANES), 1) % CAP >= CAP - 2
    message = jnp.where(carried, document_sums(pick_first, pick_second), lse)
    for k in range(out_ref.shape[0]):
        out_ref[k] = message


def merge_kernel(everyone_ref, weight_ref, out_ref):
    members = everyone_ref.shape[0]
    top = everyone_ref[0]
    total = everyone_ref[0]
    for k in range(1, members):
        top = jnp.maximum(top, everyone_ref[k])
        total = total + everyone_ref[k]
    exp_sum = jnp.zeros_like(top)
    for k in range(members):
        exp_sum = exp_sum + jnp.exp(everyone_ref[k] - top)
    lse = top + jnp.log(exp_sum)
    carried = iota((8, LANES), 1) % CAP >= CAP - 2
    lse = jnp.where(carried, 0.0, lse)
    sums = document_sums(weight_ref[0] * lse, weight_ref[1] * lse)
    group = jnp.where(carried, sums - total, 0.0)
    for k in range(out_ref.shape[0]):
        out_ref[k] = group


def select_kernel(cutoff_ref, groups_ref, log_ref, margin_ref):
    values = groups_ref[...].reshape(-1, LANES)
    across = values.T
    count = values.shape[0]
    lanes = [x * CAP + CAP - 2 + d for x in range(4) for d in range(2)]
    best = jnp.full((count, 1), jnp.inf, F32)
    for lane in lanes:
        value = values[:, lane : lane + 1]
        below = jnp.zeros((count, count), F32)
        for other in lanes:
            below = below + jnp.where(across[other : other + 1, :] <= value, 1.0, 0.0)
        rank = jnp.sum(below, axis=1, keepdims=True)
        best = jnp.minimum(
            best, jnp.where(rank >= cutoff_ref[0].astype(F32), value, jnp.inf)
        )
    threshold = jnp.min(best)
    own = groups_ref[lax.axis_index("y") * 2 + lax.axis_index("c")]
    row, lane_at = iota((8, LANES), 0), iota((8, LANES), 1)
    for d in range(2):
        here = (row == lax.axis_index("z")) & (
            lane_at == lax.axis_index("x") * CAP + CAP - 2 + d
        )
        log_ppl = jnp.sum(jnp.where(here, own, 0.0))
        log_ref[d] = log_ppl
        margin_ref[d] = log_ppl - threshold


def on_device(
    hidden_in,
    tokens,
    lengths,
    cutoff,
    norm_gain,
    gate_weight,
    up_weight,
    down_weight,
    final_gain,
    head_table,
):
    width = hidden_in.shape[2]
    shard = head_table.shape[0]
    half_shard, half = shard // 2, width // 2
    size = {axis: lax.axis_size(axis) for axis in AXES}

    sent, residual = pl.pallas_call(
        prepare_kernel,
        out_shape=(pltpu.VMEM((CAP + EXTRA, width), BF16), pltpu.VMEM((CAP, width), BF16)),
        in_specs=[SMEM, VMEM, VMEM, VMEM],
        out_specs=(VMEM, VMEM),
        cost_estimate=cost(4_000_000),
        compiler_params=params(58),
    )(lengths, tokens, hidden_in, norm_gain.reshape(1, width))
    arrived = [sent if step == 0 else shift(sent, "x", step) for step in X_STEPS]

    weights = (gate_weight, up_weight, down_weight)
    *weights, _ = lax.optimization_barrier((*weights, sent))
    weights = pl.pallas_call(
        stage_kernel,
        out_shape=tuple(pltpu.VMEM(weight.shape, BF16) for weight in weights),
        in_specs=[pl.BlockSpec(memory_space=pltpu.HBM)] * 3,
        out_specs=(VMEM,) * 3,
        scratch_shapes=[pltpu.SemaphoreType.DMA((3,))],
        cost_estimate=cost(3_000_000, 6_300_000),
        compiler_params=params(54),
    )(*weights)
    from_below = shift(head_table, "y", 1)
    from_above = shift(head_table, "y", -1)
    partials = pl.pallas_call(
        feed_kernel,
        out_shape=(
            jax.ShapeDtypeStruct((CAP, width), F32),
            *(jax.ShapeDtypeStruct((CAP, width), BF16),) * 3,
            jax.ShapeDtypeStruct((EXTRA, width), BF16),
        ),
        in_specs=[VMEM] * 7,
        out_specs=(VMEM,) * 5,
        scratch_shapes=[pltpu.VMEM((4 * CAP, width), BF16)],
        cost_estimate=cost(800_000_000, 6_300_000, 131072),
        compiler_params=params(16),
    )(*arrived, *weights)
    own_part, parts, meta = partials[0], partials[1:4], partials[4]
    returned = [shift(part, "x", -step) for part, step in zip(parts, X_STEPS[1:])]
    final_rows = pl.pallas_call(
        finish_kernel,
        out_shape=jax.ShapeDtypeStruct((CAP, width), BF16),
        in_specs=[VMEM] * 6,
        out_specs=VMEM,
        cost_estimate=cost(1_000_000),
        compiler_params=params(4),
    )(own_part, *returned, residual, final_gain.reshape(1, width))


    def joined(parts):
        rows = sum(part.shape[0] for part in parts)
        return pl.pallas_call(
            join_kernel,
            out_shape=jax.ShapeDtypeStruct((rows, width), BF16),
            in_specs=[VMEM] * len(parts),
            out_specs=VMEM,
            cost_estimate=cost(500_000),
            compiler_params=params(4),
        )(*parts)

    chunk = joined([final_rows if s == 0 else shift(final_rows, "x", s) for s in X_STEPS] + [meta])

    def step_on(below, above):
        return shift(below, "z", 1), shift(above, "z", -1)

    up_1, down_1 = step_on(chunk, chunk)
    chunk, from_below, from_above = lax.optimization_barrier((chunk, from_below, from_above))
    far = [shift(from_below[:half_shard], "y", 1), shift(from_above[half_shard:], "y", -1)]
    near_table = joined([head_table, from_below, from_above])
    near_tables = [near_table, shift(near_table, "c", 1)]
    near_steps = [((0, 3, 1), 0), ((0, 3, 1), 1)]
    far_steps = [((2,), 0), ((2,), 1)]

    def score(chunks, tables, table_steps):
        rows = len(chunks) * LANES
        entries = sum(table.shape[0] for table in tables)
        refs = [part for chunk in chunks for part in chunk]
        layout = [len(chunk) for chunk in chunks]

        def kernel(*refs):
            score_kernel(layout, table_steps, *refs)

        return pl.pallas_call(
            kernel,
            out_shape=jax.ShapeDtypeStruct((len(chunks), 8, LANES), F32),
            in_specs=[VMEM] * (len(refs) + len(tables)),
            out_specs=VMEM,
            scratch_shapes=[
                pltpu.VMEM((rows, width), BF16),
                pltpu.VMEM((len(chunks) // 2, 1, 2 * LANES), jnp.int32),
                pltpu.VMEM((len(chunks) // 2, 8, 2 * LANES), F32),
            ],
            cost_estimate=cost(2 * rows * width * entries, 2 * width * entries, rows * entries),
            compiler_params=params(24),
        )(*refs, *tables)

    up_2, down_2 = step_on(up_1, down_1)
    near = score([[up_1], [down_1]], near_tables, near_steps)
    up_2, down_2, near = lax.optimization_barrier((up_2, down_2, near))
    up_3, down_3 = step_on(up_2, down_2)
    up_2, down_2, *far = lax.optimization_barrier((up_2, down_2, *far))
    far_table = joined(far)
    far_tables = [far_table, shift(far_table, "c", 1)]
    middle = score([[up_2], [down_2]], near_tables, near_steps)
    up_3, down_3, middle = lax.optimization_barrier((up_3, down_3, middle))
    across = step_on(up_3[:, :half], down_3[:, half:])
    all_tables, all_steps = near_tables + far_tables, near_steps + far_steps
    outer = score([[up_3], [down_3]], all_tables, all_steps)
    distant = score([[up_1], [down_1], [up_2], [down_2]], far_tables, far_steps)
    across, outer, distant = lax.optimization_barrier((across, outer, distant))
    last = score([[chunk], across], all_tables, all_steps)

    members = size["z"] * size["x"]
    message, shares = pl.pallas_call(
        message_kernel,
        out_shape=(
            jax.ShapeDtypeStruct((members, 8, LANES), F32),
            jax.ShapeDtypeStruct((2, 8, LANES), F32),
        ),
        in_specs=[VMEM] * 5,
        out_specs=(VMEM, VMEM),
        cost_estimate=cost(1_000_000),
        compiler_params=params(4),
    )(near, middle, distant, outer, last)
    everyone = lax.all_to_all(message, ("z", "x"), 0, 0, tiled=True)
    groups = size["y"] * size["c"]
    group = pl.pallas_call(
        merge_kernel,
        out_shape=jax.ShapeDtypeStruct((groups, 8, LANES), F32),
        in_specs=[VMEM, VMEM],
        out_specs=VMEM,
        cost_estimate=cost(1_000_000),
        compiler_params=params(4),
    )(everyone, shares)
    group = lax.all_to_all(group, ("y", "c"), 0, 0, tiled=True)
    log_ppl, margin = pl.pallas_call(
        select_kernel,
        out_shape=(jax.ShapeDtypeStruct((2,), F32), jax.ShapeDtypeStruct((2,), F32)),
        in_specs=[SMEM, VMEM],
        out_specs=(SMEM, SMEM),
        cost_estimate=cost(1_000_000),
        compiler_params=params(4),
    )(cutoff, group)
    return (log_ppl, margin)


def solution(mesh):
    finer = Mesh(mesh.devices.reshape(8, 4, 2, mesh.shape["vocab"]), AXES)

    return jax.shard_map(
        on_device,
        mesh=finer,
        in_specs=(
            P(AXES, None, None),
            P(AXES, None),
            P(AXES),
            P(),
            P(),
            P(None, "x"),
            P(None, "x"),
            P("x", None),
            P(),
            P(AXES, None),
        ),
        out_specs=(P(AXES), P(AXES)),
        check_vma=False,
    )
```

```python
import jax
import jax.numpy as jnp
from jax import lax
from jax.experimental import pallas as pl
from jax.experimental.pallas import tpu as pltpu
from jax.sharding import Mesh
from jax.sharding import PartitionSpec as P

CAP = 32
EXTRA = 8
LANES = 4 * CAP
TILE = 256
AXES = ("z", "y", "c", "x")
X_STEPS = (0, -1, 2, 1)
HIGHEST = lax.Precision.HIGHEST
F32 = jnp.float32
BF16 = jnp.bfloat16
VMEM = pl.BlockSpec(memory_space=pltpu.VMEM)
SMEM = pl.BlockSpec(memory_space=pltpu.SMEM)


def params(mib):
    return pltpu.CompilerParams(vmem_limit_bytes=mib * 1024 * 1024)


def cost(flops, moved=0, exps=0):
    return pl.CostEstimate(flops=flops, bytes_accessed=moved, transcendentals=exps)


def shift(array, axis, step):
    length = lax.axis_size(axis)
    pairs = [(i, (i + step) % length) for i in range(length)]
    return lax.ppermute(array, axis, pairs)


def rms_norm(values, gain):
    squares = jnp.mean(values * values, axis=-1, keepdims=True)
    return values * lax.rsqrt(squares + 1e-06) * gain


def iota(shape, dim):
    return lax.broadcasted_iota(jnp.int32, shape, dim)


def prepare_kernel(lengths_ref, tokens_ref, hidden_ref, gain_ref, sent_ref, residual_ref):
    docs, length, width = hidden_ref.shape
    lives = [lengths_ref[d] - 1 for d in range(docs)]
    starts = [0, lives[0]]
    residual = jnp.zeros((CAP, width), F32)
    target = jnp.zeros((8, CAP), F32)
    slot_down, place_right = iota((CAP, length), 0), iota((CAP, length), 1)
    place_down, slot_right = iota((length, CAP), 0), iota((length, CAP), 1)
    for d in range(docs):
        live = (slot_down >= starts[d]) & (slot_down < starts[d] + lives[d])
        placing = (place_right == slot_down - starts[d]) & live
        residual = residual + jnp.dot(
            placing.astype(BF16), hidden_ref[d], preferred_element_type=F32
        )
        live = (slot_right >= starts[d]) & (slot_right < starts[d] + lives[d])
        taking = (place_down == slot_right - starts[d] + 1) & live
        token = tokens_ref[d : d + 1, :]
        digits = [token & 255, (token >> 8) & 255, token >> 16]
        digits = jnp.concatenate(digits + [jnp.zeros((5, length), jnp.int32)], axis=0)
        target = target + jnp.dot(
            digits.astype(F32).astype(BF16), taking.astype(BF16), preferred_element_type=F32
        )
    residual_ref[...] = residual.astype(BF16)
    sent_ref[:CAP, :] = rms_norm(residual, gain_ref[...]).astype(BF16)
    row, slot = iota((8, CAP), 0), iota((8, CAP), 1)
    for d in range(docs):
        live = (slot >= starts[d]) & (slot < starts[d] + lives[d]) & (row == 3 + d)
        target = jnp.where(live, lives[d].astype(F32), target)
    sent_ref[CAP:, :] = jnp.concatenate([target, jnp.zeros((8, width - CAP), F32)], axis=1).astype(
        BF16
    )


def feed_kernel(*refs):
    arrived, (gate_ref, up_ref, down_ref) = refs[:4], refs[4:7]
    own_ref, out_refs, meta_ref, rows = refs[7], refs[8:11], refs[11], refs[12]
    for k, ref in enumerate(arrived):
        rows[k * CAP : (k + 1) * CAP, :] = ref[:CAP, :]
    metas = jnp.concatenate([ref[CAP:, :CAP].astype(F32) for ref in arrived], axis=1)
    meta_ref[...] = jnp.zeros_like(meta_ref)
    meta_ref[:, :LANES] = metas.astype(BF16)
    segment = rows[...]
    units = gate_ref.shape[1]
    total = jnp.zeros((4 * CAP, down_ref.shape[1]), F32)
    for at in range(0, units, 2 * TILE):
        span = slice(at, at + 2 * TILE)
        gate = jnp.dot(segment, gate_ref[:, span], preferred_element_type=F32)
        up = jnp.dot(segment, up_ref[:, span], preferred_element_type=F32)
        active = (gate / (1.0 + jnp.exp(-gate)) * up).astype(BF16)
        total = total + jnp.dot(active, down_ref[span, :], preferred_element_type=F32)
    own_ref[...] = total[:CAP]
    for k, ref in enumerate(out_refs):
        ref[...] = total[(k + 1) * CAP : (k + 2) * CAP].astype(BF16)


def finish_kernel(own_ref, first_ref, second_ref, third_ref, residual_ref, gain_ref, out_ref):
    branch = own_ref[...] + first_ref[...].astype(F32)
    branch = branch + second_ref[...].astype(F32) + third_ref[...].astype(F32)
    stream = (residual_ref[...].astype(F32) + branch).astype(BF16)
    out_ref[...] = rms_norm(stream.astype(F32), gain_ref[...]).astype(BF16)


def join_kernel(*refs):
    out_ref, at = refs[-1], 0
    for ref in refs[:-1]:
        out_ref[at : at + ref.shape[0], :] = ref[...]
        at += ref.shape[0]


def stage_kernel(*refs):
    count = (len(refs) - 1) // 2
    copies = [
        pltpu.make_async_copy(refs[k], refs[count + k], refs[-1].at[k]) for k in range(count)
    ]
    for copy in copies:
        copy.start()
    for copy in copies:
        copy.wait()


def score_kernel(layout, table_steps, *refs):
    chunk_count, held = len(layout), sum(layout)
    chunk_refs, refs = list(refs[:held]), refs[held:]
    table_refs, (out_ref, rows, targets, results) = refs[:-4], refs[-4:]
    metas = []
    for k, parts in enumerate(layout):
        metas.append(chunk_refs[0][LANES:, :LANES].astype(F32))
        span = rows.shape[1] // parts
        for part in range(parts):
            rows[k * LANES : (k + 1) * LANES, part * span : (part + 1) * span] = chunk_refs.pop(0)[
                :LANES, :
            ]
    groups, total = chunk_count // 2, 2 * LANES
    for k, meta in enumerate(metas):
        target = meta[0:1] + 256.0 * meta[1:2] + 65536.0 * meta[2:3]
        targets[k // 2, :, (k % 2) * LANES : (k % 2 + 1) * LANES] = target.astype(jnp.int32)
    column = iota((TILE, total), 0)
    z, y, c, x = [lax.axis_index(axis) for axis in AXES]

    def score_group(group, carry):
        left = rows[pl.ds(pl.multiple_of(group * total, total), total), :]
        target = targets[group]
        peak = jnp.full((8, total), -3.0e38, F32)
        exp_sum = jnp.zeros((8, total), F32)
        picked = jnp.zeros((8, total), F32)
        for table, (y_steps, c_step) in zip(table_refs, table_steps):
            for tile in range(table.shape[0] // TILE):
                y_at, c_at = lax.rem(y + y_steps[tile // 2], 4), lax.rem(c + c_step, 2)
                shard_at = ((z * 4 + y_at) * 2 + c_at) * 4 + x
                local = target - (2 * shard_at + tile % 2) * TILE
                logits = lax.dot_general(
                    table[tile * TILE : (tile + 1) * TILE, :],
                    left,
                    (((1,), (1,)), ((), ())),
                    preferred_element_type=F32,
                )
                found = jnp.where(column == local, logits, 0.0)
                grouped = logits.reshape(TILE // 8, 8, total)
                highest = jnp.maximum(peak, jnp.max(grouped, axis=0))
                exp_sum = exp_sum * jnp.exp(peak - highest) + jnp.sum(
                    jnp.exp(grouped - highest[None]), axis=0
                )
                picked = picked + jnp.sum(found.reshape(TILE // 8, 8, total), axis=0)
                peak = highest
        top = jnp.max(peak, axis=0, keepdims=True)
        lse = top + jnp.log(jnp.sum(exp_sum * jnp.exp(peak - top), axis=0, keepdims=True))
        results[group, 0:1, :] = lse
        results[group, 1:2, :] = jnp.sum(picked, axis=0, keepdims=True)
        return carry

    if groups == 1:
        score_group(0, 0)
    else:
        lax.fori_loop(0, groups, score_group, 0)
    for k, meta in enumerate(metas):
        part = slice((k % 2) * LANES, (k % 2 + 1) * LANES)
        lse, pick = results[k // 2, 0:1, part], results[k // 2, 1:2, part]
        first, second = [
            jnp.where(line > 0.0, 1.0 / jnp.maximum(line, 1.0), 0.0)
            for line in (meta[3:4], meta[4:5])
        ]
        lines = [lse, first * pick, second * pick, first, second]
        out_ref[k] = jnp.concatenate(lines + [jnp.zeros((3, LANES), F32)], axis=0)


def document_sums(first, second):
    slot_at, lane_at = iota((LANES, LANES), 0), iota((LANES, LANES), 1)
    same = slot_at // CAP == lane_at // CAP
    sums = jnp.zeros_like(first)
    for values, lane in ((first, CAP - 2), (second, CAP - 1)):
        into = (same & (lane_at % CAP == lane)).astype(F32)
        sums = sums + jnp.dot(values, into, precision=HIGHEST, preferred_element_type=F32)
    return sums


def message_kernel(near_ref, middle_ref, far_ref, outer_ref, last_ref, out_ref, weight_ref):
    def joined(left, right):
        top = jnp.maximum(left[0:1], right[0:1])
        lse = top + jnp.log(jnp.exp(left[0:1] - top) + jnp.exp(right[0:1] - top))
        return jnp.concatenate([lse, left[1:3] + right[1:3], left[3:]], axis=0)

    near = [joined(near_ref[k], far_ref[k]) for k in range(2)]
    middle = [joined(middle_ref[k], far_ref[2 + k]) for k in range(2)]
    order = [
        last_ref[0],
        near[1],
        middle[1],
        outer_ref[1],
        last_ref[1],
        outer_ref[0],
        middle[0],
        near[0],
    ]
    kinds = [jnp.concatenate([part[k : k + 1] for part in order], axis=0) for k in range(5)]
    kinds = [
        pltpu.roll(pltpu.roll(kind, lax.axis_index("z"), 0), lax.axis_index("x") * CAP, 1)
        for kind in kinds
    ]
    lse, pick_first, pick_second, weight_first, weight_second = kinds
    weight_ref[0] = weight_first
    weight_ref[1] = weight_second
    carried = iota((8, LANES), 1) % CAP >= CAP - 2
    message = jnp.where(carried, document_sums(pick_first, pick_second), lse)
    for k in range(out_ref.shape[0]):
        out_ref[k] = message


def merge_kernel(everyone_ref, weight_ref, out_ref):
    members = everyone_ref.shape[0]
    top = everyone_ref[0]
    total = everyone_ref[0]
    for k in range(1, members):
        top = jnp.maximum(top, everyone_ref[k])
        total = total + everyone_ref[k]
    exp_sum = jnp.zeros_like(top)
    for k in range(members):
        exp_sum = exp_sum + jnp.exp(everyone_ref[k] - top)
    lse = top + jnp.log(exp_sum)
    carried = iota((8, LANES), 1) % CAP >= CAP - 2
    lse = jnp.where(carried, 0.0, lse)
    sums = document_sums(weight_ref[0] * lse, weight_ref[1] * lse)
    out_ref[...] = jnp.where(carried, sums - total, 0.0)


def select_kernel(cutoff_ref, *refs):
    groups, (log_ref, margin_ref) = refs[:-2], refs[-2:]
    values = jnp.concatenate([ref[...] for ref in groups], axis=0)
    across = values.T
    count = values.shape[0]
    lanes = [x * CAP + CAP - 2 + d for x in range(4) for d in range(2)]
    best = jnp.full((count, 1), jnp.inf, F32)
    for lane in lanes:
        value = values[:, lane : lane + 1]
        below = jnp.zeros((count, count), F32)
        for other in lanes:
            below = below + jnp.where(across[other : other + 1, :] <= value, 1.0, 0.0)
        rank = jnp.sum(below, axis=1, keepdims=True)
        best = jnp.minimum(
            best, jnp.where(rank >= cutoff_ref[0].astype(F32), value, jnp.inf)
        )
    threshold = jnp.min(best)
    own = values[:8]
    row, lane_at = iota((8, LANES), 0), iota((8, LANES), 1)
    for d in range(2):
        here = (row == lax.axis_index("z")) & (
            lane_at == lax.axis_index("x") * CAP + CAP - 2 + d
        )
        log_ppl = jnp.sum(jnp.where(here, own, 0.0))
        log_ref[d] = log_ppl
        margin_ref[d] = log_ppl - threshold


def on_device(
    hidden_in,
    tokens,
    lengths,
    cutoff,
    norm_gain,
    gate_weight,
    up_weight,
    down_weight,
    final_gain,
    head_table,
):
    width = hidden_in.shape[2]
    shard = head_table.shape[0]
    half_shard, half = shard // 2, width // 2
    size = {axis: lax.axis_size(axis) for axis in AXES}

    sent, residual = pl.pallas_call(
        prepare_kernel,
        out_shape=(pltpu.VMEM((CAP + EXTRA, width), BF16), pltpu.VMEM((CAP, width), BF16)),
        in_specs=[SMEM, VMEM, VMEM, VMEM],
        out_specs=(VMEM, VMEM),
        cost_estimate=cost(4_000_000),
        compiler_params=params(58),
    )(lengths, tokens, hidden_in, norm_gain.reshape(1, width))
    arrived = [sent if step == 0 else shift(sent, "x", step) for step in X_STEPS]

    weights = (gate_weight, up_weight, down_weight)
    *weights, _ = lax.optimization_barrier((*weights, sent))
    weights = pl.pallas_call(
        stage_kernel,
        out_shape=tuple(pltpu.VMEM(weight.shape, BF16) for weight in weights),
        in_specs=[pl.BlockSpec(memory_space=pltpu.HBM)] * 3,
        out_specs=(VMEM,) * 3,
        scratch_shapes=[pltpu.SemaphoreType.DMA((3,))],
        cost_estimate=cost(3_000_000, 6_300_000),
        compiler_params=params(54),
    )(*weights)
    from_below = shift(head_table, "y", 1)
    from_above = shift(head_table, "y", -1)
    partials = pl.pallas_call(
        feed_kernel,
        out_shape=(
            jax.ShapeDtypeStruct((CAP, width), F32),
            *(jax.ShapeDtypeStruct((CAP, width), BF16),) * 3,
            jax.ShapeDtypeStruct((EXTRA, width), BF16),
        ),
        in_specs=[VMEM] * 7,
        out_specs=(VMEM,) * 5,
        scratch_shapes=[pltpu.VMEM((4 * CAP, width), BF16)],
        cost_estimate=cost(800_000_000, 6_300_000, 131072),
        compiler_params=params(16),
    )(*arrived, *weights)
    own_part, parts, meta = partials[0], partials[1:4], partials[4]
    returned = [shift(part, "x", -step) for part, step in zip(parts, X_STEPS[1:])]
    final_rows = pl.pallas_call(
        finish_kernel,
        out_shape=jax.ShapeDtypeStruct((CAP, width), BF16),
        in_specs=[VMEM] * 6,
        out_specs=VMEM,
        cost_estimate=cost(1_000_000),
        compiler_params=params(4),
    )(own_part, *returned, residual, final_gain.reshape(1, width))


    def joined(parts):
        rows = sum(part.shape[0] for part in parts)
        return pl.pallas_call(
            join_kernel,
            out_shape=jax.ShapeDtypeStruct((rows, width), BF16),
            in_specs=[VMEM] * len(parts),
            out_specs=VMEM,
            cost_estimate=cost(500_000),
            compiler_params=params(4),
        )(*parts)

    chunk = joined([final_rows if s == 0 else shift(final_rows, "x", s) for s in X_STEPS] + [meta])

    def step_on(below, above):
        return shift(below, "z", 1), shift(above, "z", -1)

    up_1, down_1 = step_on(chunk, chunk)
    chunk, from_below, from_above = lax.optimization_barrier((chunk, from_below, from_above))
    far = [shift(from_below[:half_shard], "y", 1), shift(from_above[half_shard:], "y", -1)]
    near_table = joined([head_table, from_below, from_above])
    near_tables = [near_table, shift(near_table, "c", 1)]
    near_steps = [((0, 3, 1), 0), ((0, 3, 1), 1)]
    far_steps = [((2,), 0), ((2,), 1)]

    def score(chunks, tables, table_steps):
        rows = len(chunks) * LANES
        entries = sum(table.shape[0] for table in tables)
        refs = [part for chunk in chunks for part in chunk]
        layout = [len(chunk) for chunk in chunks]

        def kernel(*refs):
            score_kernel(layout, table_steps, *refs)

        return pl.pallas_call(
            kernel,
            out_shape=jax.ShapeDtypeStruct((len(chunks), 8, LANES), F32),
            in_specs=[VMEM] * (len(refs) + len(tables)),
            out_specs=VMEM,
            scratch_shapes=[
                pltpu.VMEM((rows, width), BF16),
                pltpu.VMEM((len(chunks) // 2, 1, 2 * LANES), jnp.int32),
                pltpu.VMEM((len(chunks) // 2, 8, 2 * LANES), F32),
            ],
            cost_estimate=cost(2 * rows * width * entries, 2 * width * entries, rows * entries),
            compiler_params=params(24),
        )(*refs, *tables)

    up_2, down_2 = step_on(up_1, down_1)
    near = score([[up_1], [down_1]], near_tables, near_steps)
    up_2, down_2, near = lax.optimization_barrier((up_2, down_2, near))
    up_3, down_3 = step_on(up_2, down_2)
    up_2, down_2, *far = lax.optimization_barrier((up_2, down_2, *far))
    far_table = joined(far)
    far_tables = [far_table, shift(far_table, "c", 1)]
    middle = score([[up_2], [down_2]], near_tables, near_steps)
    distant = score([[up_1], [down_1], [up_2], [down_2]], far_tables, far_steps)
    up_3, down_3, middle, distant = lax.optimization_barrier((up_3, down_3, middle, distant))
    across = step_on(up_3[:, :half], down_3[:, half:])
    all_tables, all_steps = near_tables + far_tables, near_steps + far_steps
    outer = score([[up_3], [down_3]], all_tables, all_steps)
    across, outer = lax.optimization_barrier((across, outer))
    last = score([[chunk], across], all_tables, all_steps)

    members = size["z"] * size["x"]
    message, shares = pl.pallas_call(
        message_kernel,
        out_shape=(
            jax.ShapeDtypeStruct((members, 8, LANES), F32),
            jax.ShapeDtypeStruct((2, 8, LANES), F32),
        ),
        in_specs=[VMEM] * 5,
        out_specs=(VMEM, VMEM),
        cost_estimate=cost(1_000_000),
        compiler_params=params(4),
    )(near, middle, distant, outer, last)
    everyone = lax.all_to_all(message, ("z", "x"), 0, 0, tiled=True)
    group = pl.pallas_call(
        merge_kernel,
        out_shape=jax.ShapeDtypeStruct((8, LANES), F32),
        in_specs=[VMEM, VMEM],
        out_specs=VMEM,
        cost_estimate=cost(1_000_000),
        compiler_params=params(4),
    )(everyone, shares)
    pair = jnp.concatenate([group, shift(group, "c", 1)], axis=0)
    log_ppl, margin = pl.pallas_call(
        select_kernel,
        out_shape=(jax.ShapeDtypeStruct((2,), F32), jax.ShapeDtypeStruct((2,), F32)),
        in_specs=[SMEM] + [VMEM] * 4,
        out_specs=(SMEM, SMEM),
        cost_estimate=cost(1_000_000),
        compiler_params=params(4),
    )(cutoff, pair, *[shift(pair, "y", step) for step in (1, -1, 2)])
    return (log_ppl, margin)


def solution(mesh):
    finer = Mesh(mesh.devices.reshape(8, 4, 2, mesh.shape["vocab"]), AXES)

    return jax.shard_map(
        on_device,
        mesh=finer,
        in_specs=(
            P(AXES, None, None),
            P(AXES, None),
            P(AXES),
            P(),
            P(),
            P(None, "x"),
            P(None, "x"),
            P("x", None),
            P(),
            P(AXES, None),
        ),
        out_specs=(P(AXES), P(AXES)),
        check_vma=False,
    )
```
